32 devices in a mesh: dp: 4 (over z), tp: 8 (over y, x, core).
Axes of the slice: x: 2, y: 2, z: 4, core: 2. Of those that a mesh axis runs over, the one named last changes fastest.
Arguments:
- tokens: bfloat16 [12, 768, 5120], P('dp'), parts along dimension 0
- positions: int32 [12, 768], P('dp'), parts along dimension 0
- lengths: int32 [12], P('dp'), parts along dimension 0
- norm_attn: bfloat16 [5120], replicated
- norm_mlp: bfloat16 [5120], replicated
- q_gain: bfloat16 [128], replicated
- k_gain: bfloat16 [128], replicated
- w_query: bfloat16 [5120, 5120], P(None, 'tp')
- w_key: bfloat16 [5120, 1024], replicated
- w_value: bfloat16 [5120, 1024], replicated
- w_out: bfloat16 [5120, 5120], P('tp')
- w_gate: bfloat16 [5120, 17408], P(None, 'tp')
- w_up: bfloat16 [5120, 17408], P(None, 'tp')
- w_down: bfloat16 [17408, 5120], P('tp')
Outputs:
- output 1: bfloat16 [12, 768, 5120], P('dp'), parts along dimension 0
- output 2: bfloat16 [12, 768, 8, 128], P('dp', None, 'tp'), parts along dimension 0
- output 3: bfloat16 [12, 768, 8, 128], P('dp', None, 'tp'), parts along dimension 0
There are 4 independent parts. The reference program is written for one: setup_inputs(seed, part) draws one part's arguments, and reference() takes and returns one part's arrays. A program takes and returns all parts, laid end to end along the dimension named above; an argument that names none is the same for every part.
All inputs are finite; a program needn't handle non-finite values.
Results may differ from the reference program's by a relative error of at most 0.0142364.
Values are sent between devices in bfloat16 or wider.
A program may use at most 1 GiB of HBM per device.

```python
import jax
import jax.numpy as jnp
from jax import lax

PROMPTS = 3
SEQ_LEN = 768
HIDDEN = 5120
Q_HEADS = 40
KV_HEADS = 8
HEAD_DIM = 128
FFN_DIM = 17408
CACHE_SLOTS = 8

EPSILON = 1e-6
ROPE_THETA = 1000000.0
GROUP_SIZE = Q_HEADS // KV_HEADS
SLOT_REPEAT = CACHE_SLOTS // KV_HEADS


def make_gain(key_gain, size_n, center, spread):
    return (center + spread * jax.random.normal(key_gain, (size_n,), jnp.float32)).astype(jnp.bfloat16)


def make_matrix(key_mat, rows_n, cols_n, scale_f):
    normal_draw = jax.random.normal(key_mat, (rows_n, cols_n), jnp.float32)
    return (normal_draw * (scale_f * rows_n ** -0.5)).astype(jnp.bfloat16)


def setup_inputs(seed: int = 0, part: int = 0) -> dict:
    part_keys = jax.random.split(jax.random.fold_in(jax.random.key(seed), part), 4)
    shared_keys = jax.random.split(jax.random.key(seed + 1), 11)
    tokens = jax.random.normal(part_keys[0], (PROMPTS, SEQ_LEN, HIDDEN), jnp.float32).astype(jnp.bfloat16)
    starts = jax.random.randint(part_keys[1], (PROMPTS, 1), 0, 1024)
    positions = (starts + jnp.arange(SEQ_LEN)[None, :]).astype(jnp.int32)
    lengths = jax.random.randint(part_keys[2], (PROMPTS,), SEQ_LEN // 4, SEQ_LEN + 1)
    full_slot = jax.random.randint(part_keys[3], (), 0, PROMPTS)
    lengths = jnp.where(jnp.arange(PROMPTS) == full_slot, SEQ_LEN, lengths).astype(jnp.int32)
    return {
        'tokens': tokens,
        'positions': positions,
        'lengths': lengths,
        'norm_attn': make_gain(shared_keys[0], HIDDEN, 1.0, 0.3),
        'norm_mlp': make_gain(shared_keys[1], HIDDEN, 1.0, 0.3),
        'q_gain': make_gain(shared_keys[2], HEAD_DIM, 1.5, 0.3),
        'k_gain': make_gain(shared_keys[3], HEAD_DIM, 1.5, 0.3),
        'w_query': make_matrix(shared_keys[4], HIDDEN, Q_HEADS * HEAD_DIM, 1.0),
        'w_key': make_matrix(shared_keys[5], HIDDEN, KV_HEADS * HEAD_DIM, 1.0),
        'w_value': make_matrix(shared_keys[6], HIDDEN, KV_HEADS * HEAD_DIM, 1.0),
        'w_out': make_matrix(shared_keys[7], Q_HEADS * HEAD_DIM, HIDDEN, 2.0),
        'w_gate': make_matrix(shared_keys[8], HIDDEN, FFN_DIM, 1.0),
        'w_up': make_matrix(shared_keys[9], HIDDEN, FFN_DIM, 1.0),
        'w_down': make_matrix(shared_keys[10], FFN_DIM, HIDDEN, 1.0),
    }


def rms_scale(values, gain_vec):
    mean_sq = jnp.mean(values * values, axis=-1, keepdims=True)
    return values * lax.rsqrt(mean_sq + EPSILON) * gain_vec.astype(jnp.float32)


def rope_rotate(values, positions):
    half_dim = HEAD_DIM // 2
    inv_freq = ROPE_THETA ** (-jnp.arange(half_dim, dtype=jnp.float32) / half_dim)
    angles = positions.astype(jnp.float32)[:, :, None] * inv_freq
    cosine = jnp.cos(angles)[:, :, None, :]
    sine_tab = jnp.sin(angles)[:, :, None, :]
    first_half = values[..., :half_dim]
    second_half = values[..., half_dim:]
    return jnp.concatenate([first_half * cosine - second_half * sine_tab, second_half * cosine + first_half * sine_tab], axis=-1)


def head_attention(head_item):
    q_head, k_head, v_head, length = head_item
    scores = jnp.dot(q_head, k_head.T, preferred_element_type=jnp.float32) * HEAD_DIM ** -0.5
    row_idx = jnp.arange(SEQ_LEN)[:, None]
    col_idx = jnp.arange(SEQ_LEN)[None, :]
    allowed = (col_idx <= row_idx) & (col_idx < length)
    attn_probs = jax.nn.softmax(jnp.where(allowed, scores, -1e30), axis=-1).astype(jnp.bfloat16)
    return jnp.dot(attn_probs, v_head, preferred_element_type=jnp.float32).astype(jnp.bfloat16)


def reference(tokens, positions, lengths, norm_attn, norm_mlp, q_gain, k_gain, w_query, w_key, w_value, w_out, w_gate, w_up, w_down):
    rows_n = PROMPTS * SEQ_LEN
    tokens_f32 = tokens.astype(jnp.float32).reshape(rows_n, HIDDEN)
    normed = rms_scale(tokens_f32, norm_attn).astype(jnp.bfloat16)
    q_proj = jnp.dot(normed, w_query, preferred_element_type=jnp.float32).reshape(PROMPTS, SEQ_LEN, Q_HEADS, HEAD_DIM)
    k_proj = jnp.dot(normed, w_key, preferred_element_type=jnp.float32).reshape(PROMPTS, SEQ_LEN, KV_HEADS, HEAD_DIM)
    v_vals = jnp.dot(normed, w_value, preferred_element_type=jnp.float32).astype(jnp.bfloat16).reshape(PROMPTS, SEQ_LEN, KV_HEADS, HEAD_DIM)
    q_rot = rope_rotate(rms_scale(q_proj, q_gain), positions).astype(jnp.bfloat16)
    k_rot = rope_rotate(rms_scale(k_proj, k_gain), positions).astype(jnp.bfloat16)
    q_items = jnp.transpose(q_rot, (0, 2, 1, 3)).reshape(PROMPTS * Q_HEADS, SEQ_LEN, HEAD_DIM)
    k_items = jnp.transpose(jnp.repeat(k_rot, GROUP_SIZE, axis=2), (0, 2, 1, 3)).reshape(PROMPTS * Q_HEADS, SEQ_LEN, HEAD_DIM)
    v_items = jnp.transpose(jnp.repeat(v_vals, GROUP_SIZE, axis=2), (0, 2, 1, 3)).reshape(PROMPTS * Q_HEADS, SEQ_LEN, HEAD_DIM)
    len_items = jnp.repeat(lengths, Q_HEADS)
    attn_items = lax.map(head_attention, (q_items, k_items, v_items, len_items))
    attn_rows = jnp.transpose(attn_items.reshape(PROMPTS, Q_HEADS, SEQ_LEN, HEAD_DIM), (0, 2, 1, 3)).reshape(rows_n, Q_HEADS * HEAD_DIM)
    attn_out = jnp.dot(attn_rows, w_out, preferred_element_type=jnp.float32)
    hidden = (tokens_f32 + attn_out).astype(jnp.bfloat16).astype(jnp.float32)
    normed_mlp = rms_scale(hidden, norm_mlp).astype(jnp.bfloat16)
    gate_proj = jnp.dot(normed_mlp, w_gate, preferred_element_type=jnp.float32)
    up_proj = jnp.dot(normed_mlp, w_up, preferred_element_type=jnp.float32)
    gated = (jax.nn.silu(gate_proj) * up_proj).astype(jnp.bfloat16)
    down_proj = jnp.dot(gated, w_down, preferred_element_type=jnp.float32)
    output = (hidden + down_proj).astype(jnp.bfloat16).reshape(PROMPTS, SEQ_LEN, HIDDEN)
    valid_mask = (jnp.arange(SEQ_LEN)[None, :] < lengths[:, None])[:, :, None, None]
    k_cache = jnp.repeat(jnp.where(valid_mask, k_rot, 0).astype(jnp.bfloat16), SLOT_REPEAT, axis=2)
    v_cache = jnp.repeat(jnp.where(valid_mask, v_vals, 0).astype(jnp.bfloat16), SLOT_REPEAT, axis=2)
    return output, k_cache, v_cache
```

```python
import functools
import jax
import jax.numpy as jnp
from jax import lax
from jax.experimental import pallas as pl
from jax.experimental.pallas import tpu as pltpu
from jax.sharding import PartitionSpec as P

EPSILON = 1e-6
ROPE_THETA = 1000000.0
MESH = pl.DeviceIdType.MESH
F32, BF16 = jnp.float32, jnp.bfloat16
SLOTS = ((0, 0, 0), (0, 1, 0), (0, 0, 1), (0, 1, 1), (1, 0, 0), (1, 0, 1), (1, 1, 0), (1, 1, 1))


def rms_scale(values, gain_vec):
    mean_sq = jnp.mean(values * values, axis=-1, keepdims=True)
    return values * lax.rsqrt(mean_sq + EPSILON) * gain_vec.astype(F32)


def rope_tables(positions, half_dim):
    inv_freq = ROPE_THETA ** (-jnp.arange(half_dim, dtype=F32) / half_dim)
    angles = positions.astype(F32)[:, :, None] * inv_freq
    return jnp.cos(angles)[:, :, None, :], jnp.sin(angles)[:, :, None, :]


def rope_apply(values, cosine, sine_tab):
    half_dim = values.shape[-1] // 2
    first_half = values[..., :half_dim]
    second_half = values[..., half_dim:]
    return jnp.concatenate([first_half * cosine - second_half * sine_tab, second_half * cosine + first_half * sine_tab], axis=-1)


def local_attention(q_rot, k_rot, v_vals, lengths):
    seq_len, head_dim = k_rot.shape[1], k_rot.shape[2]
    scores = jnp.einsum('bshd,btd->bhst', q_rot, k_rot, preferred_element_type=F32) * head_dim ** -0.5
    row_idx = jnp.arange(seq_len)[:, None]
    col_idx = jnp.arange(seq_len)[None, :]
    allowed = (col_idx <= row_idx)[None, None] & (col_idx[None, None] < lengths[:, None, None, None])
    attn_probs = jax.nn.softmax(jnp.where(allowed, scores, -1e30), axis=-1).astype(BF16)
    return jnp.einsum('bhst,btd->bshd', attn_probs, v_vals, preferred_element_type=F32).astype(BF16)


def flip(t, bit):
    return t + bit - 2 * bit * lax.rem(lax.div(t, bit), 2)


def origin_block(t, slot):
    part, dy, dx = SLOTS[slot % 8]
    owner = t
    if slot >= 8:
        owner = flip(owner, 1)
    if dx:
        owner = flip(owner, 2)
    if dy:
        owner = flip(owner, 4)
    return 2 * owner + part


def stage_kernel(cfg, *refs):
    kind, ars, steps, width, rows, ffn_tile = cfg['kind'], cfg['ars'], cfg['steps'], cfg['width'], cfg['rows'], cfg['ffn_tile']
    piece = rows // 16
    half = rows // 2
    quarter = rows // 8
    it = iter(refs)
    take = lambda: next(it)
    n_chunks = len(cfg['chunks'])
    if kind == 'mlp':
        lhs_hbm, wg_hbm, wu_hbm, wd_ref = take(), take(), take(), take()
    elif kind == 'wout':
        lhs_hbm, wo_ref = take(), take()
    ar_in = []
    for ar in ars:
        d = dict(own=take(), rcv=take(), res=take())
        if ar['kind'] == 'attn':
            d['gain'] = take()
        ar_in.append(d)
    out_own, out_rcv = [], []
    for _ in range(n_chunks):
        out_own.append(take())
        out_rcv.append(take())
    for d, ar in zip(ar_in, ars):
        d['g'] = take()
        if ar['kind'] == 'attn':
            d['h'] = take()
    if kind == 'mlp':
        lhs, gated, wbuf, w_sem = take(), take(), take(), take()
    elif kind == 'wout':
        lhs = take()
    if n_chunks:
        obuf, lhs_sem, o_sem, os_sem, or_sem = take(), take(), take(), take(), take()
    for d, ar in zip(ar_in, ars):
        for name in ('s', 'r', 'r1', 'r2', 'x', 'n', 'send', 'recv', 'loc'):
            d[name] = take()

    t = lax.axis_index('tp')
    core, xn, yn = {'tp': flip(t, 1)}, {'tp': flip(t, 2)}, {'tp': flip(t, 4)}
    step = pl.program_id(0)

    def rcopy(d, i, src, dst, dev):
        return pltpu.make_async_remote_copy(src_ref=src, dst_ref=dst, send_sem=d['send'].at[i], recv_sem=d['recv'].at[i], device_id=dev, device_id_type=MESH)

    def lcopy(sem, src, dst):
        return pltpu.make_async_copy(src, dst, sem)

    def at(ref, start, n):
        return ref.at[pl.ds(start, n)]

    def slots(d, first, n=1):
        return at(d['g'], first * piece, n * piece)

    def ar_loads(d, ar):
        if ar['kind'] == 'attn':
            res = at(d['res'], ar['chunk'] * rows + pl.multiple_of(t * quarter, quarter), quarter)
        else:
            res = d['res']
        return [lcopy(d['loc'].at[0], d['own'], d['s']), lcopy(d['loc'].at[1], d['rcv'], d['r']), lcopy(d['loc'].at[2], res, d['x'])]

    def p1(d):
        return [rcopy(d, 0, at(d['s'], quarter, quarter), d['r1'].at[0], xn), rcopy(d, 1, at(d['s'], 3 * quarter, quarter), d['r1'].at[1], yn)]

    def p2(d):
        return [rcopy(d, 2, at(d['s'], piece, piece), d['r2'].at[0], yn), rcopy(d, 3, at(d['s'], 2 * quarter + piece, piece), d['r2'].at[1], xn)]

    def p3(d):
        a, b = at(d['n'], 0, piece), at(d['n'], piece, piece)
        return [rcopy(d, 4, a, slots(d, 1), yn), rcopy(d, 5, b, slots(d, 5), xn), rcopy(d, 6, a, slots(d, 2), xn), rcopy(d, 7, b, slots(d, 6), yn),
                rcopy(d, 10, a, slots(d, 8), core), rcopy(d, 11, b, slots(d, 12), core)]

    def own_out(d):
        return [lcopy(d['loc'].at[3], at(d['n'], 0, piece), slots(d, 0)), lcopy(d['loc'].at[4], at(d['n'], piece, piece), slots(d, 4))]

    def h_out(d):
        return lcopy(d['loc'].at[5], d['x'], d['h'])

    def p4(d):
        return [rcopy(d, 8, slots(d, 1), slots(d, 3), xn), rcopy(d, 9, slots(d, 5), slots(d, 7), yn)]

    def c1(d):
        return [rcopy(d, 12, slots(d, 1, 2), slots(d, 9, 2), core), rcopy(d, 13, slots(d, 5, 2), slots(d, 13, 2), core)]

    def c2(d):
        return [rcopy(d, 14, slots(d, 3), slots(d, 11), core), rcopy(d, 15, slots(d, 7), slots(d, 15), core)]

    def add_rows(dst, dst0, src, src0, n):
        def body(i, _):
            a = pl.ds(pl.multiple_of(dst0 + i * 16, 16), 16)
            b = pl.ds(pl.multiple_of(src0 + i * 16, 16), 16)
            dst[a, :] = (dst[a, :].astype(F32) + src[b, :].astype(F32)).astype(BF16)
            return 0
        lax.fori_loop(0, n // 16, body, 0)

    def ar_start_loads():
        for d, ar in zip(ar_in, ars):
            for cp in ar_loads(d, ar):
                cp.start()

    def ar_phase1():
        for d, ar in zip(ar_in, ars):
            for cp in ar_loads(d, ar):
                cp.wait()
            add_rows(d['s'], quarter, d['r'], quarter, quarter)
            p1(d)[0].start()
            add_rows(d['s'], 3 * quarter, d['r'], 3 * quarter, quarter)
            p1(d)[1].start()
            add_rows(d['s'], 0, d['r'], 0, quarter)
            add_rows(d['s'], 2 * quarter, d['r'], 2 * quarter, quarter)

    def ar_phase2():
        for d in ar_in:
            a, b = p1(d)
            a.wait_recv()
            add_rows(d['s'], piece, d['r1'].at[0], piece, piece)
            p2(d)[0].start()
            b.wait_recv()
            add_rows(d['s'], 2 * quarter + piece, d['r1'].at[1], piece, piece)
            p2(d)[1].start()
            add_rows(d['s'], 0, d['r1'].at[0], 0, piece)
            add_rows(d['s'], 2 * quarter, d['r1'].at[1], 0, piece)

    def ar_finish(d, ar, part):
        base = part * piece
        src0 = part * 2 * quarter

        def body(i, _):
            here = pl.ds(pl.multiple_of(base + i * 16, 16), 16)
            there = pl.ds(pl.multiple_of(src0 + i * 16, 16), 16)
            other = pl.ds(pl.multiple_of(i * 16, 16), 16)
            total = d['s'][there, :].astype(F32) + d['r2'][part, other, :].astype(F32)
            hid = (d['x'][here, :].astype(F32) + total).astype(BF16)
            if ar['kind'] == 'attn':
                d['x'][here, :] = hid
                hid = hid.astype(F32)
                mean_sq = jnp.sum(hid * hid, axis=-1, keepdims=True) / width
                hid = (hid * lax.rsqrt(mean_sq + EPSILON) * d['gain'][...].astype(F32)).astype(BF16)
            d['n'][here, :] = hid
            return 0
        lax.fori_loop(0, piece // 16, body, 0)

    def ar_phase3():
        for d, ar in zip(ar_in, ars):
            cps = p3(d)
            rec = p2(d)
            rec[0].wait_recv()
            ar_finish(d, ar, 0)
            cps[0].start()
            rec[1].wait_recv()
            ar_finish(d, ar, 1)
            for cp in cps[1:]:
                cp.start()
            for cp in own_out(d):
                cp.start()
            if ar['kind'] == 'attn':
                h_out(d).start()

    def ar_phase4():
        for d in ar_in:
            cps = p3(d)
            fwd = p4(d)
            cps[0].wait_recv()
            fwd[0].start()
            cps[1].wait_recv()
            fwd[1].start()

    def ar_end():
        for d in ar_in:
            cps, cc = p3(d), c1(d)
            cps[2].wait_recv()
            cc[0].start()
            cps[3].wait_recv()
            cc[1].start()
        for d in ar_in:
            fwd, cc = p4(d), c2(d)
            fwd[0].wait_recv()
            cc[0].start()
            fwd[1].wait_recv()
            cc[1].start()
        for d, ar in zip(ar_in, ars):
            cps = p3(d)
            cps[4].wait_recv()
            cps[5].wait_recv()
            for cp in c1(d) + c2(d):
                cp.wait_recv()
            for cp in p1(d) + p2(d) + p3(d) + p4(d) + c1(d) + c2(d):
                cp.wait_send()
            for cp in own_out(d):
                cp.wait()
            if ar['kind'] == 'attn':
                h_out(d).wait()

    def w_copies(j):
        slot = lax.rem(j, 2)
        cols = pl.ds(pl.multiple_of(j * ffn_tile, ffn_tile), ffn_tile)
        return [lcopy(w_sem.at[slot, 0], wg_hbm.at[:, cols], wbuf.at[slot, :, pl.ds(0, ffn_tile)]),
                lcopy(w_sem.at[slot, 1], wu_hbm.at[:, cols], wbuf.at[slot, :, pl.ds(ffn_tile, ffn_tile)])]

    def lhs_copies():
        if kind == 'mlp':
            return [lcopy(lhs_sem.at[0], lhs_hbm, lhs)]
        out = []
        for ci, chunk in enumerate(cfg['chunks']):
            for s in range(16):
                src = at(lhs_hbm, chunk * rows + pl.multiple_of(origin_block(t, s) * piece, piece), piece)
                out.append(lcopy(lhs_sem.at[ci * 16 + s], src, lhs.at[ci, pl.ds(s * piece, piece)]))
        return out

    def tile_copies(ci, j, slot):
        n = obuf.shape[2]
        cols = pl.ds(pl.multiple_of(j * n, n), n)
        return (lcopy(o_sem.at[slot], obuf.at[slot, pl.ds(0, half)], out_own[ci].at[:, cols]),
                pltpu.make_async_remote_copy(src_ref=obuf.at[slot, pl.ds(half, half)], dst_ref=out_rcv[ci].at[:, cols],
                                             send_sem=os_sem.at[slot], recv_sem=or_sem.at[ci], device_id=core, device_id_type=MESH))

    n_steps = cfg['n_steps']

    @pl.when(step == 0)
    def _():
        ar_start_loads()
        if n_chunks:
            for cp in lhs_copies():
                cp.start()
        if kind == 'mlp':
            for cp in w_copies(0):
                cp.start()
        barrier = pltpu.get_barrier_semaphore()
        for dev in (core, xn, yn):
            pl.semaphore_signal(barrier, inc=1, device_id=dev, device_id_type=MESH)
        pl.semaphore_wait(barrier, 3)
        ar_phase1()
        if n_chunks:
            for cp in lhs_copies():
                cp.wait()

    if ars:
        for at_step, phase in zip(steps, (ar_phase2, ar_phase3, ar_phase4)):
            pl.when(step == at_step)(phase)

    def store_tile(ci, j, count, value):
        slot = lax.rem(count, 2)

        @pl.when(count >= 2)
        def _():
            a, b = tile_copies(ci, j, slot)
            a.wait()
            b.wait_send()
        obuf[slot] = value
        a, b = tile_copies(ci, j, slot)
        a.start()
        b.start()

    if kind == 'mlp':
        n_up = cfg['n_up']

        @pl.when(step < n_up)
        def _():
            @pl.when(step + 1 < n_up)
            def _():
                for cp in w_copies(step + 1):
                    cp.start()
            for cp in w_copies(step):
                cp.wait()
            both = jnp.dot(lhs[...], wbuf[lax.rem(step, 2)], preferred_element_type=F32)
            gate = both[:, :ffn_tile]
            gated[:, pl.ds(pl.multiple_of(step * ffn_tile, ffn_tile), ffn_tile)] = (gate * jax.nn.sigmoid(gate) * both[:, ffn_tile:]).astype(BF16)

        @pl.when(step >= n_up)
        def _():
            store_tile(0, step - n_up, step - n_up, jnp.dot(gated[...], wd_ref[...], preferred_element_type=F32).astype(BF16))
    elif kind == 'wout':
        per = cfg['per']
        for ci in range(n_chunks):
            @pl.when(lax.div(step, per) == ci)
            def _(ci=ci):
                store_tile(ci, step - ci * per, step, jnp.dot(lhs[ci], wo_ref[...], preferred_element_type=F32).astype(BF16))

    @pl.when(step == n_steps - 1)
    def _():
        if n_chunks:
            per = cfg['per']
            for j in (per - 2, per - 1):
                a, b = tile_copies(n_chunks - 1, j, ((n_chunks - 1) * per + j) % 2)
                a.wait()
                b.wait_send()
            for ci in range(n_chunks):
                pltpu.make_async_copy(out_rcv[ci], out_rcv[ci], or_sem.at[ci]).wait()
        ar_end()


def run_stage(cid, kind, compute, ars, steps, rows, width, chunks=()):
    any_spec = pl.BlockSpec(memory_space=pl.ANY)
    half, quarter, piece = rows // 2, rows // 8, rows // 16
    args, in_specs, out_shape, scratch = [], [], [], []
    out_tile = 512 if width % 512 == 0 else 128
    per = width // out_tile
    cfg = dict(kind=kind, steps=steps, width=width, rows=rows, chunks=chunks, per=per, ffn_tile=128,
               ars=[dict(kind=a['kind'], chunk=a['chunk']) for a in ars])
    if kind == 'mlp':
        n2, wg, wu, wd = compute
        ffn = wd.shape[0]
        n_up = ffn // 128
        cfg.update(n_up=n_up, n_steps=n_up + per)
        args += [n2, wg, wu, wd]
        in_specs += [any_spec] * 3 + [pl.BlockSpec((ffn, out_tile), lambda j: (0, jnp.maximum(j - n_up, 0)))]
        scratch += [pltpu.VMEM((rows, width), BF16), pltpu.VMEM((rows, ffn), BF16), pltpu.VMEM((2, width, 256), BF16), pltpu.SemaphoreType.DMA((2, 2))]
        n_lhs = 1
    elif kind == 'wout':
        o, wo = compute
        cfg.update(n_steps=per * len(chunks))
        args += [o, wo]
        in_specs += [any_spec, pl.BlockSpec((wo.shape[0], out_tile), lambda j: (0, lax.rem(j, per)))]
        scratch += [pltpu.VMEM((len(chunks), rows, wo.shape[0]), BF16)]
        n_lhs = 16 * len(chunks)
    else:
        cfg.update(n_steps=max(steps) + 1)
    if chunks:
        scratch += [pltpu.VMEM((2, rows, out_tile), BF16), pltpu.SemaphoreType.DMA((n_lhs,)), pltpu.SemaphoreType.DMA((2,)),
                    pltpu.SemaphoreType.DMA((2,)), pltpu.SemaphoreType.DMA((len(chunks),))]
    for a in ars:
        args += [a['own'], a['rcv'], a['res']]
        in_specs += [any_spec] * 3
        if a['kind'] == 'attn':
            args.append(a['gain'])
            in_specs.append(pl.BlockSpec((1, width), lambda j: (0, 0)))
        scratch += [pltpu.VMEM((half, width), BF16), pltpu.VMEM((half, width), BF16), pltpu.VMEM((2, quarter, width), BF16),
                    pltpu.VMEM((2, piece, width), BF16), pltpu.VMEM((quarter, width), BF16), pltpu.VMEM((quarter, width), BF16),
                    pltpu.SemaphoreType.DMA((16,)), pltpu.SemaphoreType.DMA((16,)), pltpu.SemaphoreType.DMA((6,))]
    for _ in chunks:
        out_shape += [jax.ShapeDtypeStruct((half, width), BF16)] * 2
    for a in ars:
        out_shape.append(jax.ShapeDtypeStruct((rows, width), BF16))
        if a['kind'] == 'attn':
            out_shape.append(jax.ShapeDtypeStruct((quarter, width), BF16))
    return pl.pallas_call(
        functools.partial(stage_kernel, cfg),
        grid=(cfg['n_steps'],),
        out_shape=out_shape,
        in_specs=in_specs,
        out_specs=[any_spec] * len(out_shape),
        scratch_shapes=scratch,
        compiler_params=pltpu.CompilerParams(collective_id=cid, has_side_effects=True, vmem_limit_bytes=62 * 1024 * 1024,
                                             dimension_semantics=('arbitrary',)),
        name=f'stage{cid}',
    )(*args)


def place_kernel(n, table_ref, *refs):
    for b in range(n):
        refs[n][b] = refs[b][...]


def place_rows(chunks, rows, width):
    t = lax.axis_index('tp')
    piece = rows // 16
    blocks = jnp.stack([jnp.asarray(origin_block(t, s), jnp.int32) for s in range(16)])
    table = jnp.argmax(blocks[None, :] == jnp.arange(16, dtype=jnp.int32)[:, None], axis=1).astype(jnp.int32)
    n = len(chunks)
    return pl.pallas_call(
        functools.partial(place_kernel, n),
        grid_spec=pltpu.PrefetchScalarGridSpec(
            num_scalar_prefetch=1, grid=(16,),
            in_specs=[pl.BlockSpec((piece, width), lambda k, tab: (tab[k], 0))] * n,
            out_specs=pl.BlockSpec((n, piece, width), lambda k, tab: (0, k, 0))),
        out_shape=jax.ShapeDtypeStruct((n, rows, width), BF16),
        name='place',
    )(table, *chunks)


def layer_body(tokens, positions, lengths, norm_attn, norm_mlp, q_gain, k_gain, w_query, w_key, w_value, w_out, w_gate, w_up, w_down, tp_size):
    num_prompts, seq_len, hidden_dim = tokens.shape
    head_dim = q_gain.shape[0]
    local_heads = w_query.shape[1] // head_dim
    kv_heads = w_key.shape[1] // head_dim
    kv_index = lax.axis_index('tp') // (tp_size // kv_heads)
    rows_n = num_prompts * seq_len
    tokens_flat = tokens.reshape(rows_n, hidden_dim)
    normed = rms_scale(tokens_flat.astype(F32), norm_attn).astype(BF16)
    w_key_head = lax.dynamic_slice_in_dim(w_key, kv_index * head_dim, head_dim, axis=1)
    w_value_head = lax.dynamic_slice_in_dim(w_value, kv_index * head_dim, head_dim, axis=1)
    q_proj = jnp.dot(normed, w_query, preferred_element_type=F32).reshape(num_prompts, seq_len, local_heads, head_dim)
    k_proj = jnp.dot(normed, w_key_head, preferred_element_type=F32).reshape(num_prompts, seq_len, 1, head_dim)
    v_vals = jnp.dot(normed, w_value_head, preferred_element_type=F32).astype(BF16).reshape(num_prompts, seq_len, head_dim)
    cosine, sine_tab = rope_tables(positions, head_dim // 2)
    q_rot = rope_apply(rms_scale(q_proj, q_gain), cosine, sine_tab).astype(BF16)
    k_rot = rope_apply(rms_scale(k_proj, k_gain), cosine, sine_tab).astype(BF16).reshape(num_prompts, seq_len, head_dim)
    valid_mask = (jnp.arange(seq_len)[None, :] < lengths[:, None])[:, :, None]
    k_cache = jnp.where(valid_mask, k_rot, 0).astype(BF16)[:, :, None, :]
    v_cache = jnp.where(valid_mask, v_vals, 0).astype(BF16)[:, :, None, :]
    attn_rows = local_attention(q_rot, k_rot, v_vals, lengths).reshape(rows_n, local_heads * head_dim)

    gain = norm_mlp.reshape(1, hidden_dim)
    stage = functools.partial(run_stage, rows=seq_len, width=hidden_dim)

    def attn_ar(chunk, own, rcv):
        return dict(kind='attn', chunk=chunk, own=own, rcv=rcv, res=tokens_flat, gain=gain)

    def mlp_ar(own, rcv, hid):
        return dict(kind='mlp', chunk=0, own=own, rcv=rcv, res=hid)

    weights = (w_gate, w_up, w_down)
    own0, rcv0 = stage(1, 'wout', (attn_rows, w_out), [], (), chunks=(0,))
    own1, rcv1, own2, rcv2, n0, h0 = stage(2, 'wout', (attn_rows, w_out), [attn_ar(0, own0, rcv0)], (17, 18, 19), chunks=(1, 2))
    m_own0, m_rcv0, n1, h1 = stage(3, 'mlp', (n0, *weights), [attn_ar(1, own1, rcv1)], (11, 16, 22), chunks=(0,))
    m_own1, m_rcv1, n2, h2, out0 = stage(4, 'mlp', (n1, *weights), [attn_ar(2, own2, rcv2), mlp_ar(m_own0, m_rcv0, h0)], (20, 25, 26), chunks=(1,))
    m_own2, m_rcv2, out1 = stage(5, 'mlp', (n2, *weights), [mlp_ar(m_own1, m_rcv1, h1)], (11, 16, 22), chunks=(2,))
    out2, = stage(6, 'none', (), [mlp_ar(m_own2, m_rcv2, h2)], (0, 1, 2))
    output = place_rows([out0, out1, out2], seq_len, hidden_dim)
    return output, k_cache, v_cache


def solution(mesh):
    body = functools.partial(layer_body, tp_size=mesh.shape['tp'])
    in_specs = (P('dp', None, None), P('dp', None), P('dp'), P(), P(), P(), P(), P(None, 'tp'), P(), P(), P('tp', None), P(None, 'tp'), P(None, 'tp'), P('tp', None))
    out_specs = (P('dp', None, None), P('dp', None, 'tp', None), P('dp', None, 'tp', None))
    return jax.shard_map(body, mesh=mesh, in_specs=in_specs, out_specs=out_specs, check_vma=False)
```

```python
import functools
import jax
import jax.numpy as jnp
from jax import lax
from jax.experimental import pallas as pl
from jax.experimental.pallas import tpu as pltpu
from jax.sharding import PartitionSpec as P

EPSILON = 1e-6
ROPE_THETA = 1000000.0
MESH = pl.DeviceIdType.MESH
END = 1000
F32, BF16 = jnp.float32, jnp.bfloat16
SLOTS = ((0, 0, 0), (0, 1, 0), (0, 0, 1), (0, 1, 1), (1, 0, 0), (1, 0, 1), (1, 1, 0), (1, 1, 1))


def rope_tables(positions, half_dim):
    inv_freq = ROPE_THETA ** (-jnp.arange(half_dim, dtype=F32) / half_dim)
    angles = positions.astype(F32).reshape(-1, 1) * inv_freq
    cosine, sine = jnp.cos(angles), jnp.sin(angles)
    return jnp.concatenate([cosine, cosine], axis=-1), jnp.concatenate([-sine, sine], axis=-1)


class Lazy:
    def __init__(self, make):
        self.make = make

    def start(self):
        self.make().start()

    def wait(self):
        self.make().wait()

    def wait_send(self):
        self.make().wait_send()

    def wait_recv(self):
        self.make().wait_recv()


def flip(t, bit):
    return t + bit - 2 * bit * lax.rem(lax.div(t, bit), 2)


def origin_block(t, slot):
    part, dy, dx = SLOTS[slot % 8]
    owner = t
    if slot >= 8:
        owner = flip(owner, 1)
    if dx:
        owner = flip(owner, 2)
    if dy:
        owner = flip(owner, 4)
    return 2 * owner + part


def ar_scratch(do):
    return (() if do == 'ag' else ('s', 'r', 'r1', 'r2')) + (() if do == 'rs' else ('x',)) + ('n', 'send', 'recv', 'loc')


def stage_kernel(cfg, *refs):
    kind, ars, width, rows, ffn_tile = cfg['kind'], cfg['ars'], cfg['width'], cfg['rows'], cfg['ffn_tile']
    piece = rows // 16
    half = rows // 2
    quarter = rows // 8
    it = iter(refs)
    take = lambda: next(it)
    n_chunks = len(cfg['chunks'])
    if kind == 'mlp':
        lhs_hbm, wg_hbm, wu_hbm, wd_ref = take(), take(), take(), take()
    elif kind == 'head':
        len_ref, x_hbm, wq_hbm, wk_hbm, wv_hbm, norm_ref, qg_ref, kg_ref, cos_ref, sin_ref, wo_ref = (take() for _ in range(11))
    ar_in = []
    for ar in ars:
        d = {}
        if ar['do'] != 'ag' and ar['source'] is None:
            d.update(own=take(), rcv=take())
        if ar['do'] == 'ag':
            d['sum'] = take()
        if ar['do'] != 'rs':
            d['res'] = take()
            if ar['kind'] == 'attn':
                d['gain'] = take()
        ar_in.append(d)
    out_own, out_rcv = [], []
    for _ in range(n_chunks):
        out_own.append(take())
        out_rcv.append(take())
    if kind == 'head':
        kc_ref, vc_ref = take(), take()
    for d, ar in zip(ar_in, ars):
        if ar['source'] is not None:
            d.update(own=out_own[ar['source']], rcv=out_rcv[ar['source']])
        if ar['do'] == 'rs':
            d['sum'] = take()
        else:
            d['g'] = take()
            if ar['kind'] == 'attn':
                d['h'] = take()
    if kind == 'mlp':
        lhs, lhs_sem, gated, wbuf, w_sem = take(), take(), take(), take(), take()
    elif kind == 'head':
        lhs, x_sem, m_buf, w_a, w_b, w_sem, q_buf, k_buf, v_buf, o_buf = (take() for _ in range(10))
    if n_chunks:
        obuf, o_sem, os_sem, or_sem = take(), take(), take(), take()
    for d, ar in zip(ar_in, ars):
        for name in ar_scratch(ar['do']):
            d[name] = take()

    t = lax.axis_index('tp')
    core, xn, yn = {'tp': flip(t, 1)}, {'tp': flip(t, 2)}, {'tp': flip(t, 4)}
    step = pl.program_id(0)

    def rcopy(d, i, src, dst, dev):
        return Lazy(lambda: pltpu.make_async_remote_copy(src_ref=src, dst_ref=dst, send_sem=d['send'].at[i], recv_sem=d['recv'].at[i], device_id=dev, device_id_type=MESH))

    def lcopy(sem, src, dst):
        return Lazy(lambda: pltpu.make_async_copy(src, dst, sem))

    def at(ref, start, n):
        return ref.at[pl.ds(start, n)]

    def slots(d, first, n=1):
        return at(d['g'], first * piece, n * piece)

    def sum_loads(d, ar):
        out = []
        if ar['do'] == 'ag':
            return out
        for i, q in enumerate((1, 3, 0, 2)):
            for k, (src, dst) in enumerate(((d['own'], d['s']), (d['rcv'], d['r']))):
                out.append(lcopy(d['loc'].at[2 * i + k], at(src, q * quarter, quarter), at(dst, q * quarter, quarter)))
        return out

    def row_loads(d, ar):
        if ar['do'] == 'rs':
            return []
        if ar['kind'] == 'attn':
            res = at(d['res'], ar['chunk'] * rows + pl.multiple_of(t * quarter, quarter), quarter)
        else:
            res = d['res']
        out = [lcopy(d['loc'].at[8], res, d['x'])]
        if ar['do'] == 'ag':
            out.append(lcopy(d['loc'].at[0], d['sum'], d['n']))
        return out

    def sum_out(d):
        return lcopy(d['loc'].at[9], d['n'], d['sum'])

    def p1(d):
        def part(i, first, which, lo, dev):
            return rcopy(d, i, at(d['s'], first + lo, piece), d['r1'].at[which, pl.ds(lo, piece)], dev)
        return [part(0, quarter, 0, piece, xn), part(1, 3 * quarter, 1, piece, yn), part(16, quarter, 0, 0, xn), part(17, 3 * quarter, 1, 0, yn)]

    def p2(d):
        return [rcopy(d, 2, at(d['s'], piece, piece), d['r2'].at[0], yn), rcopy(d, 3, at(d['s'], 2 * quarter + piece, piece), d['r2'].at[1], xn)]

    def p3(d):
        a, b = at(d['n'], 0, piece), at(d['n'], piece, piece)
        return [rcopy(d, 4, a, slots(d, 1), yn), rcopy(d, 5, b, slots(d, 5), xn), rcopy(d, 6, a, slots(d, 2), xn), rcopy(d, 7, b, slots(d, 6), yn),
                rcopy(d, 10, a, slots(d, 8), core), rcopy(d, 11, b, slots(d, 12), core)]

    def own_out(d):
        return [lcopy(d['loc'].at[9], at(d['n'], 0, piece), slots(d, 0)), lcopy(d['loc'].at[10], at(d['n'], piece, piece), slots(d, 4))]

    def h_out(d):
        return lcopy(d['loc'].at[11], d['x'], d['h'])

    def p4(d):
        return [rcopy(d, 8, slots(d, 1), slots(d, 3), xn), rcopy(d, 9, slots(d, 5), slots(d, 7), yn)]

    def c1(d):
        return [rcopy(d, 12, slots(d, 1, 2), slots(d, 9, 2), core), rcopy(d, 13, slots(d, 5, 2), slots(d, 13, 2), core)]

    def c2(d):
        return [rcopy(d, 14, slots(d, 3), slots(d, 11), core), rcopy(d, 15, slots(d, 7), slots(d, 15), core)]

    def add_rows(dst, dst0, src, src0, n):
        def body(i, _):
            a = pl.ds(pl.multiple_of(dst0 + i * 16, 16), 16)
            b = pl.ds(pl.multiple_of(src0 + i * 16, 16), 16)
            dst[a, :] = (dst[a, :].astype(F32) + src[b, :].astype(F32)).astype(BF16)
            return 0
        lax.fori_loop(0, n // 16, body, 0)

    def ar_phase1(d, ar):
        loads, sends = sum_loads(d, ar), p1(d)
        for k, q in enumerate((1, 3)):
            loads[2 * k].wait()
            loads[2 * k + 1].wait()
            add_rows(d['s'], q * quarter + piece, d['r'], q * quarter + piece, piece)
            sends[k].start()
        for k, q in enumerate((1, 3)):
            add_rows(d['s'], q * quarter, d['r'], q * quarter, piece)
            sends[2 + k].start()
        for cp in loads[4:]:
            cp.wait()
        add_rows(d['s'], 0, d['r'], 0, quarter)
        add_rows(d['s'], 2 * quarter, d['r'], 2 * quarter, quarter)

    def ar_phase2(d, ar):
        for k in range(2):
            p1(d)[k].wait_recv()
            add_rows(d['s'], 2 * k * quarter + piece, d['r1'].at[k], piece, piece)
            p2(d)[k].start()

    def ar_finish(d, ar, part):
        base = part * piece
        src0 = part * 2 * quarter

        def body(i, _):
            here = pl.ds(pl.multiple_of(base + i * 16, 16), 16)
            there = pl.ds(pl.multiple_of(src0 + i * 16, 16), 16)
            other = pl.ds(pl.multiple_of(i * 16, 16), 16)
            if ar['do'] == 'ag':
                total = d['n'][here, :].astype(F32)
            else:
                total = d['s'][there, :].astype(F32) + d['r2'][part, other, :].astype(F32)
            if ar['do'] == 'rs':
                d['n'][here, :] = total.astype(BF16)
                return 0
            hid = (d['x'][here, :].astype(F32) + total).astype(BF16)
            if ar['kind'] == 'attn':
                d['x'][here, :] = hid
                hid = hid.astype(F32)
                mean_sq = jnp.sum(hid * hid, axis=-1, keepdims=True) / width
                hid = (hid * lax.rsqrt(mean_sq + EPSILON) * d['gain'][...].astype(F32)).astype(BF16)
            d['n'][here, :] = hid
            return 0
        lax.fori_loop(0, piece // 16, body, 0)

    def ar_phase3(d, ar):
        if ar['do'] != 'ag':
            for k in range(2):
                p1(d)[2 + k].wait_recv()
                add_rows(d['s'], 2 * k * quarter, d['r1'].at[k], 0, piece)
        for cp in row_loads(d, ar):
            cp.wait()
        for part in range(2):
            if ar['do'] != 'ag':
                p2(d)[part].wait_recv()
            ar_finish(d, ar, part)
            if ar['do'] != 'rs':
                p3(d)[part].start()
        if ar['do'] == 'rs':
            sum_out(d).start()
            return
        for cp in p3(d)[2:] + own_out(d):
            cp.start()
        if ar['kind'] == 'attn':
            h_out(d).start()

    def ar_phase4(d, ar):
        for k in range(2):
            p3(d)[k].wait_recv()
            p4(d)[k].start()

    def ar_phase5(d, ar):
        for k in range(2):
            p3(d)[2 + k].wait_recv()
            c1(d)[k].start()

    def ar_phase6(d, ar):
        for k in range(2):
            p4(d)[k].wait_recv()
            c2(d)[k].start()

    def ar_end(d, ar):
        if ar['do'] == 'rs':
            sum_out(d).wait()
        else:
            for cp in p3(d)[4:] + c1(d) + c2(d):
                cp.wait_recv()
            for cp in p3(d) + p4(d) + c1(d) + c2(d):
                cp.wait_send()
            for cp in own_out(d):
                cp.wait()
            if ar['kind'] == 'attn':
                h_out(d).wait()
        if ar['do'] != 'ag':
            for cp in p1(d) + p2(d):
                cp.wait_send()

    phase_sets = {'full': (ar_phase1, ar_phase2, ar_phase3, ar_phase4, ar_phase5, ar_phase6), 'rs': (ar_phase1, ar_phase2, ar_phase3),
                  'ag': (ar_phase3, ar_phase4, ar_phase5, ar_phase6)}

    def run_phases(k):
        for d, ar in zip(ar_in, ars):
            for when, phase in zip(ar['steps'], phase_sets[ar['do']]):
                if when == k:
                    phase(d, ar)

    def w_copies(j, n):
        slot = lax.rem(j, 2)
        cols = pl.ds(j * ffn_tile if isinstance(j, int) else pl.multiple_of(j * ffn_tile, ffn_tile), n)
        return [lcopy(w_sem.at[slot, 0], wg_hbm.at[:, cols], wbuf.at[slot, :, pl.ds(0, n)]),
                lcopy(w_sem.at[slot, 1], wu_hbm.at[:, cols], wbuf.at[slot, :, pl.ds(n, n)])]

    def lhs_copies():
        return [lcopy(lhs_sem.at[0], lhs_hbm, lhs)]

    def tile_copies(ci, j, slot):
        n = obuf.shape[2]
        cols = pl.ds(pl.multiple_of(j * n, n), n)
        return (lcopy(o_sem.at[slot], obuf.at[slot, pl.ds(0, half)], out_own[ci].at[:, cols]),
                Lazy(lambda: pltpu.make_async_remote_copy(src_ref=obuf.at[slot, pl.ds(half, half)], dst_ref=out_rcv[ci].at[:, cols],
                                             send_sem=os_sem.at[slot], recv_sem=or_sem.at[ci], device_id=core, device_id_type=MESH)))

    n_steps = cfg['n_steps']
    if kind == 'head':
        x_tile, heads, first = cfg['x_tile'], cfg['heads'], cfg['chunks'][0]
        tiles = rows // x_tile
        na = cfg['na']

    def x_copies(ci):
        return [lcopy(x_sem.at[i], at(x_hbm, pl.multiple_of((first + ci) * rows + i * x_tile, x_tile), x_tile), at(m_buf, i * x_tile, x_tile)) for i in range(tiles)]

    def qkv_copies():
        kv = pl.ds(pl.multiple_of(lax.div(t, cfg['kv_share']) * 128, 128), 128)
        cut, rest = na * 128, (heads - na) * 128
        return [lcopy(w_sem.at[0], wq_hbm.at[:, pl.ds(0, cut)], w_a), lcopy(w_sem.at[1], wq_hbm.at[:, pl.ds(cut, rest)], w_b.at[:, pl.ds(0, rest)]),
                lcopy(w_sem.at[2], wk_hbm.at[:, kv], w_b.at[:, pl.ds(rest, 128)]), lcopy(w_sem.at[3], wv_hbm.at[:, kv], w_b.at[:, pl.ds(rest + 128, 128)])]

    def norm_step(ci):
        cps = x_copies(ci)
        for tile in range(tiles):
            cps[tile].wait()

            def norm_rows(i, _):
                here = pl.ds(pl.multiple_of(tile * x_tile + i * 16, 16), 16)
                val = m_buf[here, :].astype(F32)
                mean_sq = jnp.sum(val * val, axis=-1, keepdims=True) / width
                m_buf[here, :] = (val * lax.rsqrt(mean_sq + EPSILON) * norm_ref[...].astype(F32)).astype(BF16)
                return 0
            lax.fori_loop(0, x_tile // 16, norm_rows, 0)

    def rotate(val, gain_ref):
        val = val * lax.rsqrt(jnp.sum(val * val, axis=-1, keepdims=True) / 128 + EPSILON) * gain_ref[...].astype(F32)
        return (val * cos_ref[...] + pltpu.roll(val, 64, 1) * sin_ref[...]).astype(BF16)

    def masked(ci, val):
        row = lax.broadcasted_iota(jnp.int32, (rows, 128), 0)
        return jnp.where(row < len_ref[first + ci], val.astype(F32), 0.0).astype(BF16)

    def query_step():
        proj = jnp.dot(m_buf[...], w_a[...], preferred_element_type=F32)
        for i in range(na):
            q_buf[i] = rotate(proj[:, i * 128:(i + 1) * 128], qg_ref)

    def last_step(ci):
        proj = jnp.dot(m_buf[...], w_b[...], preferred_element_type=F32)
        for i in range(na, heads):
            q_buf[i] = rotate(proj[:, (i - na) * 128:(i - na + 1) * 128], qg_ref)
        rest = (heads - na) * 128
        key = rotate(proj[:, rest:rest + 128], kg_ref)
        k_buf[...] = key
        kc_ref[...] = masked(ci, key)
        val = proj[:, rest + 128:].astype(BF16)
        v_buf[...] = val
        vc_ref[...] = masked(ci, val)

    def attention_step(ci, h):
        length = len_ref[first + ci]
        for i in range(tiles):
            n = (i + 1) * x_tile
            q = q_buf[h, i * x_tile:n, :]
            scores = lax.dot_general(q, k_buf[:n, :], (((1,), (1,)), ((), ())), preferred_element_type=F32) * 128 ** -0.5
            row = lax.broadcasted_iota(jnp.int32, (x_tile, n), 0) + i * x_tile
            col = lax.broadcasted_iota(jnp.int32, (x_tile, n), 1)
            scores = jnp.where((col <= row) & (col < length), scores, -1e30)
            weight = jnp.exp(scores - jnp.max(scores, axis=-1, keepdims=True))
            weight = (weight * (1.0 / jnp.sum(weight, axis=-1, keepdims=True))).astype(BF16)
            out = jnp.dot(weight, v_buf[:n, :], preferred_element_type=F32).astype(BF16)
            o_buf[i * x_tile:n, pl.ds(pl.multiple_of(h * 128, 128), 128)] = out

    def order_rows():
        for s in range(16):
            src = pl.ds(pl.multiple_of(origin_block(t, s) * piece, 16), piece)
            lhs[s * piece:(s + 1) * piece, :] = o_buf[src, :]

    @pl.when(step == 0)
    def _():
        for d, ar in zip(ar_in, ars):
            for cp in ([] if ar['source'] is not None else sum_loads(d, ar)) + row_loads(d, ar):
                cp.start()
        if kind == 'mlp':
            for cp in lhs_copies() + w_copies(0, ffn_tile):
                cp.start()
        if kind == 'head':
            for cp in x_copies(0) + qkv_copies():
                cp.start()
        barrier = pltpu.get_barrier_semaphore()
        for dev in (core, xn, yn):
            pl.semaphore_signal(barrier, inc=1, device_id=dev, device_id_type=MESH)
        pl.semaphore_wait(barrier, 3)
        run_phases(0)
        if kind == 'mlp':
            for cp in lhs_copies():
                cp.wait()

    for k in sorted({k for ar in ars for k in ar['steps']} - {0, END}):
        @pl.when(step == k)
        def _(k=k):
            run_phases(k)

    def drain(ci):
        for j in (cfg['per'] - 2, cfg['per'] - 1):
            a, b = tile_copies(ci, j, j % 2)
            a.wait()
            b.wait_send()
        pltpu.make_async_copy(out_rcv[ci], out_rcv[ci], or_sem.at[ci]).wait()

    def store_tile(ci, j, value):
        slot = lax.rem(j, 2)

        @pl.when(j >= 2)
        def _():
            a, b = tile_copies(ci, j, slot)
            a.wait()
            b.wait_send()
        obuf[slot] = value
        a, b = tile_copies(ci, j, slot)
        a.start()
        b.start()

    if kind == 'mlp':
        n_up = cfg['n_up']

        n_full, rest = cfg['n_full'], cfg['rest']

        @pl.when(step + 1 < n_full)
        def _():
            for cp in w_copies(step + 1, ffn_tile):
                cp.start()

        def gate_up(j, n):
            for cp in w_copies(j, n):
                cp.wait()
            both = jnp.dot(lhs[...], wbuf[lax.rem(j, 2), :, :2 * n], preferred_element_type=F32)
            gate = both[:, :n]
            gated[:, pl.ds(j * ffn_tile if isinstance(j, int) else pl.multiple_of(j * ffn_tile, ffn_tile), n)] = (gate * jax.nn.sigmoid(gate) * both[:, n:]).astype(BF16)

        if rest:
            @pl.when(step == n_full - 1)
            def _():
                for cp in w_copies(n_full, rest):
                    cp.start()

        @pl.when(step < n_full)
        def _():
            gate_up(step, ffn_tile)
        if rest:
            @pl.when(step == n_full)
            def _():
                gate_up(n_full, rest)

        @pl.when(step >= n_up)
        def _():
            store_tile(0, step - n_up, jnp.dot(gated[...], wd_ref[...], preferred_element_type=F32).astype(BF16))
    elif kind == 'head':
        per = cfg['per']
        ci = lax.div(step, cfg['chunk_steps'])
        sub = lax.rem(step, cfg['chunk_steps'])
        for c in range(n_chunks - 1):
            @pl.when(step == (c + 1) * cfg['chunk_steps'])
            def _(c=c):
                drain(c)
                for d, ar in zip(ar_in, ars):
                    if ar['source'] == c:
                        for cp in sum_loads(d, ar):
                            cp.start()

        begin = 2

        @pl.when(sub == 0)
        def _():
            norm_step(ci)
        for b, part in enumerate((slice(0, 1), slice(1, 4))):
            @pl.when(step == b)
            def _(part=part):
                for cp in qkv_copies()[part]:
                    cp.wait()
        pl.when(sub == 0)(query_step)

        @pl.when(sub == 1)
        def _():
            last_step(ci)

        @pl.when((sub == begin) & (ci + 1 < n_chunks))
        def _():
            for cp in x_copies(ci + 1):
                cp.start()

        @pl.when((sub >= begin) & (sub < begin + heads))
        def _():
            attention_step(ci, sub - begin)
        pl.when(sub == begin + heads)(order_rows)

        @pl.when(sub >= begin + heads)
        def _():
            value = jnp.dot(lhs[...], wo_ref[...], preferred_element_type=F32).astype(BF16)
            j = sub - begin - heads
            for c in range(n_chunks):
                @pl.when(ci == c)
                def _(c=c):
                    store_tile(c, j, value)

    @pl.when(step == n_steps - 1)
    def _():
        if n_chunks:
            drain(n_chunks - 1)
        for phase in (ar_phase1, ar_phase2, ar_phase3, ar_phase4, ar_phase5, ar_phase6):
            for d, ar in zip(ar_in, ars):
                for when, own_phase in zip(ar['steps'], phase_sets[ar['do']]):
                    if when == END and own_phase is phase:
                        phase(d, ar)
        for d, ar in zip(ar_in, ars):
            ar_end(d, ar)


def run_stage(cid, kind, compute, ars, rows, width, chunks=(), kv_share=1):
    any_spec = pl.BlockSpec(memory_space=pl.ANY)
    half, quarter, piece = rows // 2, rows // 8, rows // 16
    args, in_specs, out_shape, scratch = [], [], [], []
    out_tile = 512 if width % 512 == 0 else 128
    per = width // out_tile
    cfg = dict(kind=kind, width=width, rows=rows, chunks=chunks, per=per, ffn_tile=256,
               ars=[{k: a[k] for k in ('kind', 'chunk', 'do', 'steps', 'source')} for a in ars])
    if kind == 'mlp':
        n2, wg, wu, wd = compute
        ffn = wd.shape[0]
        n_full, rest = ffn // 256, ffn % 256
        n_up = n_full + (rest > 0)
        cfg.update(n_up=n_up, n_full=n_full, rest=rest, n_steps=n_up + per)
        args += [n2, wg, wu, wd]
        in_specs += [any_spec] * 3 + [pl.BlockSpec((ffn, out_tile), lambda j: (0, jnp.maximum(j - n_up, 0)))]
        scratch += [pltpu.VMEM((rows, width), BF16), pltpu.SemaphoreType.DMA((1,)), pltpu.VMEM((rows, ffn), BF16), pltpu.VMEM((2, width, 512), BF16), pltpu.SemaphoreType.DMA((2, 2))]
    elif kind == 'head':
        lengths, tokens, wq, wk, wv, norm, q_gain, k_gain, cosine, sine, wo = compute
        x_tile = rows // 3
        heads = wq.shape[1] // 128
        out_tile = 1024 if width % 1024 == 0 else out_tile
        per = width // out_tile
        begin = 2
        na = heads - 1
        chunk_steps = begin + heads + per
        first = chunks[0]
        cfg.update(n_steps=chunk_steps * len(chunks), x_tile=x_tile, heads=heads, chunk_steps=chunk_steps, kv_share=kv_share, per=per, na=na)
        args += [lengths, tokens, wq, wk, wv, norm, q_gain, k_gain, cosine, sine, wo]
        table = pl.BlockSpec((rows, 128), lambda j: (first + lax.div(j, chunk_steps), 0))
        gain_spec = pl.BlockSpec((1, 128), lambda j: (0, 0))
        in_specs += [pl.BlockSpec(memory_space=pltpu.SMEM)] + [any_spec] * 4 + [pl.BlockSpec((1, width), lambda j: (0, 0)), gain_spec, gain_spec, table, table,
                     pl.BlockSpec((heads * 128, out_tile), lambda j: (0, jnp.maximum(lax.rem(j, chunk_steps) - begin - heads, 0)))]
        scratch += [pltpu.VMEM((rows, heads * 128), BF16), pltpu.SemaphoreType.DMA((3,)), pltpu.VMEM((rows, width), BF16),
                    pltpu.VMEM((width, na * 128), BF16), pltpu.VMEM((width, (heads - na) * 128 + 256), BF16), pltpu.SemaphoreType.DMA((4,)),
                    pltpu.VMEM((heads, rows, 128), BF16), pltpu.VMEM((rows, 128), BF16), pltpu.VMEM((rows, 128), BF16), pltpu.VMEM((rows, heads * 128), BF16)]
        cache_spec = pl.BlockSpec((rows, 128), lambda j: (lax.div(j, chunk_steps), 0))
    else:
        cfg.update(n_steps=3)
    if chunks:
        scratch += [pltpu.VMEM((2, rows, out_tile), BF16), pltpu.SemaphoreType.DMA((2,)),
                    pltpu.SemaphoreType.DMA((2,)), pltpu.SemaphoreType.DMA((len(chunks),))]
    for a in ars:
        names = (() if a['do'] == 'ag' or a['source'] is not None else ('own', 'rcv')) + (('sum',) if a['do'] == 'ag' else ()) + (() if a['do'] == 'rs' else ('res',))
        args += [a[k] for k in names]
        in_specs += [any_spec] * len(names)
        if a['kind'] == 'attn' and a['do'] != 'rs':
            args.append(a['gain'])
            in_specs.append(pl.BlockSpec((1, width), lambda j: (0, 0)))
        sizes = dict(s=(half, width), r=(half, width), r1=(2, quarter, width), r2=(2, piece, width), x=(quarter, width), n=(quarter, width))
        counts = dict(send=18, recv=18, loc=12)
        scratch += [pltpu.VMEM(sizes[k], BF16) if k in sizes else pltpu.SemaphoreType.DMA((counts[k],)) for k in ar_scratch(a['do'])]
    for _ in chunks:
        out_shape += [jax.ShapeDtypeStruct((half, width), BF16)] * 2
    out_specs = [any_spec] * len(out_shape)
    if kind == 'head':
        out_shape += [jax.ShapeDtypeStruct((rows * len(chunks), 128), BF16)] * 2
        out_specs += [cache_spec] * 2
    for a in ars:
        if a['do'] == 'rs':
            out_shape.append(jax.ShapeDtypeStruct((quarter, width), BF16))
            continue
        out_shape.append(jax.ShapeDtypeStruct((rows, width), BF16))
        if a['kind'] == 'attn':
            out_shape.append(jax.ShapeDtypeStruct((quarter, width), BF16))
    return pl.pallas_call(
        functools.partial(stage_kernel, cfg),
        grid=(cfg['n_steps'],),
        out_shape=out_shape,
        in_specs=in_specs,
        out_specs=out_specs + [any_spec] * (len(out_shape) - len(out_specs)),
        scratch_shapes=scratch,
        compiler_params=pltpu.CompilerParams(collective_id=cid, has_side_effects=True, vmem_limit_bytes=62 * 1024 * 1024,
                                             dimension_semantics=('arbitrary',)),
        name=f'stage{cid}',
    )(*args)


def place_kernel(n, table_ref, *refs):
    for b in range(n):
        refs[n][b] = refs[b][...]


def place_rows(chunks, rows, width):
    t = lax.axis_index('tp')
    piece = rows // 16
    blocks = jnp.stack([jnp.asarray(origin_block(t, s), jnp.int32) for s in range(16)])
    table = jnp.argmax(blocks[None, :] == jnp.arange(16, dtype=jnp.int32)[:, None], axis=1).astype(jnp.int32)
    n = len(chunks)
    return pl.pallas_call(
        functools.partial(place_kernel, n),
        grid_spec=pltpu.PrefetchScalarGridSpec(
            num_scalar_prefetch=1, grid=(16,),
            in_specs=[pl.BlockSpec((piece, width), lambda k, tab: (tab[k], 0))] * n,
            out_specs=pl.BlockSpec((n, piece, width), lambda k, tab: (0, k, 0))),
        out_shape=jax.ShapeDtypeStruct((n, rows, width), BF16),
        name='place',
    )(table, *chunks)


def layer_body(tokens, positions, lengths, norm_attn, norm_mlp, q_gain, k_gain, w_query, w_key, w_value, w_out, w_gate, w_up, w_down, tp_size):
    num_prompts, seq_len, hidden_dim = tokens.shape
    head_dim = q_gain.shape[0]
    kv_heads = w_key.shape[1] // head_dim
    rows_n = num_prompts * seq_len
    tokens_flat = tokens.reshape(rows_n, hidden_dim)
    cosine, sine = rope_tables(positions, head_dim // 2)
    head_in = (lengths, tokens_flat, w_query, w_key, w_value, norm_attn.reshape(1, hidden_dim), q_gain.reshape(1, head_dim), k_gain.reshape(1, head_dim), cosine, sine, w_out)

    gain = norm_mlp.reshape(1, hidden_dim)
    stage = functools.partial(run_stage, rows=seq_len, width=hidden_dim, kv_share=tp_size // kv_heads)

    def attn_ar(do, chunk, steps, source=None, **arrays):
        return dict(kind='attn', do=do, chunk=chunk, steps=steps, source=source, res=tokens_flat, gain=gain, **arrays)

    def mlp_ar(steps, own, rcv, hid):
        return dict(kind='mlp', do='full', chunk=0, steps=steps, source=None, own=own, rcv=rcv, res=hid)

    weights = (w_gate, w_up, w_down)
    own0, rcv0, kc0, vc0 = stage(1, 'head', head_in, [], chunks=(0,))
    _, _, own2, rcv2, kc1, vc1, n0, h0, sum1 = stage(2, 'head', head_in, [
        attn_ar('full', 0, (0, 1, 11, 13, 15, 18), own=own0, rcv=rcv0), attn_ar('rs', 1, (13, 19, END), source=0)], chunks=(1, 2))
    m_own0, m_rcv0, sum2, n1, h1 = stage(3, 'mlp', (n0, *weights), [
        attn_ar('rs', 2, (0, 2, END), own=own2, rcv=rcv2), attn_ar('ag', 1, (0, 6, END, END), sum=sum1)], chunks=(0,))
    m_own1, m_rcv1, out0, n2, h2 = stage(4, 'mlp', (n1, *weights), [
        mlp_ar((0, 2, 10, END, END, END), m_own0, m_rcv0, h0), attn_ar('ag', 2, (0, 6, END, END), sum=sum2)], chunks=(1,))
    m_own2, m_rcv2, out1 = stage(5, 'mlp', (n2, *weights), [mlp_ar((0, 2, 7, 11, END, END), m_own1, m_rcv1, h1)], chunks=(2,))
    out2, = stage(6, 'none', (), [mlp_ar((0, 0, 1, 2, END, END), m_own2, m_rcv2, h2)])
    k_parts, v_parts = [kc0, kc1], [vc0, vc1]
    cache_shape = (num_prompts, seq_len, 1, head_dim)
    k_cache = jnp.concatenate(k_parts).reshape(cache_shape)
    v_cache = jnp.concatenate(v_parts).reshape(cache_shape)
    output = place_rows([out0, out1, out2], seq_len, hidden_dim)
    return output, k_cache, v_cache


def solution(mesh):
    body = functools.partial(layer_body, tp_size=mesh.shape['tp'])
    in_specs = (P('dp', None, None), P('dp', None), P('dp'), P(), P(), P(), P(), P(None, 'tp'), P(), P(), P('tp', None), P(None, 'tp'), P(None, 'tp'), P('tp', None))
    out_specs = (P('dp', None, None), P('dp', None, 'tp', None), P('dp', None, 'tp', None))
    return jax.shard_map(body, mesh=mesh, in_specs=in_specs, out_specs=out_specs, check_vma=False)
```

```python
import functools
import jax
import jax.numpy as jnp
from jax import lax
from jax.experimental import pallas as pl
from jax.experimental.pallas import tpu as pltpu
from jax.sharding import PartitionSpec as P

EPSILON = 1e-6
ROPE_THETA = 1000000.0
MESH = pl.DeviceIdType.MESH
END = 1000
F32, BF16 = jnp.float32, jnp.bfloat16
SLOTS = ((0, 0, 0), (0, 1, 0), (0, 0, 1), (0, 1, 1), (1, 0, 0), (1, 0, 1), (1, 1, 0), (1, 1, 1))


def rope_tables(positions, half_dim):
    inv_freq = ROPE_THETA ** (-jnp.arange(half_dim, dtype=F32) / half_dim)
    angles = positions.astype(F32).reshape(-1, 1) * inv_freq
    cosine, sine = jnp.cos(angles), jnp.sin(angles)
    return jnp.concatenate([cosine, cosine], axis=-1), jnp.concatenate([-sine, sine], axis=-1)


class Lazy:
    def __init__(self, make):
        self.make = make

    def start(self):
        self.make().start()

    def wait(self):
        self.make().wait()

    def wait_send(self):
        self.make().wait_send()

    def wait_recv(self):
        self.make().wait_recv()


def flip(t, bit):
    return t + bit - 2 * bit * lax.rem(lax.div(t, bit), 2)


def origin_block(t, slot):
    part, dy, dx = SLOTS[slot % 8]
    owner = t
    if slot >= 8:
        owner = flip(owner, 1)
    if dx:
        owner = flip(owner, 2)
    if dy:
        owner = flip(owner, 4)
    return 2 * owner + part


def ar_scratch(do):
    return (() if do == 'ag' else ('s', 'r', 'r1', 'r2')) + (() if do == 'rs' else ('x',)) + ('n', 'send', 'recv', 'loc')


def stage_kernel(cfg, *refs):
    kind, ars, width, rows, ffn_tile = cfg['kind'], cfg['ars'], cfg['width'], cfg['rows'], cfg['ffn_tile']
    piece = rows // 16
    half = rows // 2
    quarter = rows // 8
    it = iter(refs)
    take = lambda: next(it)
    n_chunks = len(cfg['chunks'])
    if kind == 'mlp':
        lhs_hbm, wg_hbm, wu_hbm, wd_ref = take(), take(), take(), take()
    elif kind == 'head':
        len_ref, x_hbm, wq_hbm, wk_hbm, wv_hbm, norm_ref, qg_ref, kg_ref, cos_ref, sin_ref, wo_ref = (take() for _ in range(11))
    ar_in = []
    for ar in ars:
        d = {}
        if ar['do'] != 'ag' and ar['source'] is None:
            d.update(own=take(), rcv=take())
        if ar['do'] == 'ag':
            d['sum'] = take()
        if ar['do'] != 'rs':
            d['res'] = take()
            if ar['kind'] == 'attn':
                d['gain'] = take()
        ar_in.append(d)
    out_own, out_rcv = [], []
    for _ in range(n_chunks):
        out_own.append(take())
        out_rcv.append(take())
    if kind == 'head':
        kc_ref, vc_ref = take(), take()
    for d, ar in zip(ar_in, ars):
        if ar['source'] is not None:
            d.update(own=out_own[ar['source']], rcv=out_rcv[ar['source']])
        if ar['do'] == 'rs':
            d['sum'] = take()
        else:
            d['g'] = take()
            if ar['kind'] == 'attn':
                d['h'] = take()
    if kind == 'mlp':
        lhs, lhs_sem, gated, wbuf, w_sem = take(), take(), take(), take(), take()
    elif kind == 'head':
        lhs, x_sem, m_buf, w_a, w_b, w_sem, q_buf, k_buf, v_buf, o_buf = (take() for _ in range(10))
    if n_chunks:
        obuf, o_sem, os_sem, or_sem = take(), take(), take(), take()
    for d, ar in zip(ar_in, ars):
        for name in ar_scratch(ar['do']):
            d[name] = take()

    t = lax.axis_index('tp')
    core, xn, yn = {'tp': flip(t, 1)}, {'tp': flip(t, 2)}, {'tp': flip(t, 4)}
    step = pl.program_id(0)

    def rcopy(d, i, src, dst, dev):
        return Lazy(lambda: pltpu.make_async_remote_copy(src_ref=src, dst_ref=dst, send_sem=d['send'].at[i], recv_sem=d['recv'].at[i], device_id=dev, device_id_type=MESH))

    def lcopy(sem, src, dst):
        return Lazy(lambda: pltpu.make_async_copy(src, dst, sem))

    def at(ref, start, n):
        return ref.at[pl.ds(start, n)]

    def slots(d, first, n=1):
        return at(d['g'], first * piece, n * piece)

    def sum_loads(d, ar):
        out = []
        if ar['do'] == 'ag':
            return out
        for i, q in enumerate((1, 3, 0, 2)):
            for k, (src, dst) in enumerate(((d['own'], d['s']), (d['rcv'], d['r']))):
                out.append(lcopy(d['loc'].at[2 * i + k], at(src, q * quarter, quarter), at(dst, q * quarter, quarter)))
        return out

    def row_loads(d, ar):
        if ar['do'] == 'rs':
            return []
        if ar['kind'] == 'attn':
            res = at(d['res'], ar['chunk'] * rows + pl.multiple_of(t * quarter, quarter), quarter)
        else:
            res = d['res']
        out = [lcopy(d['loc'].at[8], res, d['x'])]
        if ar['do'] == 'ag':
            out.append(lcopy(d['loc'].at[0], d['sum'], d['n']))
        return out

    def sum_out(d):
        return lcopy(d['loc'].at[9], d['n'], d['sum'])

    def p1(d):
        def part(i, first, which, lo, dev):
            return rcopy(d, i, at(d['s'], first + lo, piece), d['r1'].at[which, pl.ds(lo, piece)], dev)
        return [part(0, quarter, 0, piece, xn), part(1, 3 * quarter, 1, piece, yn), part(16, quarter, 0, 0, xn), part(17, 3 * quarter, 1, 0, yn)]

    def p2(d):
        return [rcopy(d, 2, at(d['s'], piece, piece), d['r2'].at[0], yn), rcopy(d, 3, at(d['s'], 2 * quarter + piece, piece), d['r2'].at[1], xn)]

    def p3(d):
        a, b = at(d['n'], 0, piece), at(d['n'], piece, piece)
        return [rcopy(d, 4, a, slots(d, 1), yn), rcopy(d, 5, b, slots(d, 5), xn), rcopy(d, 6, a, slots(d, 2), xn), rcopy(d, 7, b, slots(d, 6), yn),
                rcopy(d, 10, a, slots(d, 8), core), rcopy(d, 11, b, slots(d, 12), core)]

    def own_out(d):
        return [lcopy(d['loc'].at[9], at(d['n'], 0, piece), slots(d, 0)), lcopy(d['loc'].at[10], at(d['n'], piece, piece), slots(d, 4))]

    def h_out(d):
        return lcopy(d['loc'].at[11], d['x'], d['h'])

    def p4(d):
        return [rcopy(d, 8, slots(d, 1), slots(d, 3), xn), rcopy(d, 9, slots(d, 5), slots(d, 7), yn)]

    def c1(d):
        return [rcopy(d, 12, slots(d, 1, 2), slots(d, 9, 2), core), rcopy(d, 13, slots(d, 5, 2), slots(d, 13, 2), core)]

    def c2(d):
        return [rcopy(d, 14, slots(d, 3), slots(d, 11), core), rcopy(d, 15, slots(d, 7), slots(d, 15), core)]

    def add_rows(dst, dst0, src, src0, n):
        cols_n = width // 4 if width % 512 == 0 else width

        def body(i, _):
            row, col = lax.div(i, width // cols_n) * 16, lax.rem(i, width // cols_n) * cols_n
            a = pl.ds(pl.multiple_of(dst0 + row, 16), 16)
            b = pl.ds(pl.multiple_of(src0 + row, 16), 16)
            c = pl.ds(pl.multiple_of(col, 128), cols_n)
            dst[a, c] = (dst[a, c].astype(F32) + src[b, c].astype(F32)).astype(BF16)
            return 0
        lax.fori_loop(0, n // 16 * (width // cols_n), body, 0)

    def ar_phase1(d, ar):
        loads, sends = sum_loads(d, ar), p1(d)
        for k, q in enumerate((1, 3)):
            loads[2 * k].wait()
            loads[2 * k + 1].wait()
            add_rows(d['s'], q * quarter + piece, d['r'], q * quarter + piece, piece)
            sends[k].start()
        for k, q in enumerate((1, 3)):
            add_rows(d['s'], q * quarter, d['r'], q * quarter, piece)
            sends[2 + k].start()
        for cp in loads[4:]:
            cp.wait()
        add_rows(d['s'], 0, d['r'], 0, quarter)
        add_rows(d['s'], 2 * quarter, d['r'], 2 * quarter, quarter)

    def ar_phase2(d, ar):
        for k in range(2):
            p1(d)[k].wait_recv()
            add_rows(d['s'], 2 * k * quarter + piece, d['r1'].at[k], piece, piece)
            p2(d)[k].start()

    def ar_finish(d, ar, part):
        base = part * piece
        src0 = part * 2 * quarter

        def body(i, _):
            here = pl.ds(pl.multiple_of(base + i * 16, 16), 16)
            there = pl.ds(pl.multiple_of(src0 + i * 16, 16), 16)
            other = pl.ds(pl.multiple_of(i * 16, 16), 16)
            if ar['do'] == 'ag':
                total = d['n'][here, :].astype(F32)
            else:
                total = d['s'][there, :].astype(F32) + d['r2'][part, other, :].astype(F32)
            if ar['do'] == 'rs':
                d['n'][here, :] = total.astype(BF16)
                return 0
            hid = (d['x'][here, :].astype(F32) + total).astype(BF16)
            if ar['kind'] == 'attn':
                d['x'][here, :] = hid
                hid = hid.astype(F32)
                mean_sq = jnp.sum(hid * hid, axis=-1, keepdims=True) / width
                hid = (hid * lax.rsqrt(mean_sq + EPSILON) * d['gain'][...].astype(F32)).astype(BF16)
            d['n'][here, :] = hid
            return 0
        lax.fori_loop(0, piece // 16, body, 0)

    def ar_phase3(d, ar):
        if ar['do'] != 'ag':
            for k in range(2):
                p1(d)[2 + k].wait_recv()
                add_rows(d['s'], 2 * k * quarter, d['r1'].at[k], 0, piece)
        for cp in row_loads(d, ar):
            cp.wait()
        for part in range(2):
            if ar['do'] != 'ag':
                p2(d)[part].wait_recv()
            ar_finish(d, ar, part)
            if ar['do'] != 'rs':
                p3(d)[part].start()
        if ar['do'] == 'rs':
            sum_out(d).start()
            return
        for cp in p3(d)[2:] + own_out(d):
            cp.start()
        if ar['kind'] == 'attn':
            h_out(d).start()

    def ar_phase4(d, ar):
        for k in range(2):
            p3(d)[k].wait_recv()
            p4(d)[k].start()

    def ar_phase5(d, ar):
        for k in range(2):
            p3(d)[2 + k].wait_recv()
            c1(d)[k].start()

    def ar_phase6(d, ar):
        for k in range(2):
            p4(d)[k].wait_recv()
            c2(d)[k].start()

    def ar_end(d, ar):
        if ar['do'] == 'rs':
            sum_out(d).wait()
        else:
            for cp in p3(d)[4:] + c1(d) + c2(d):
                cp.wait_recv()
            for cp in p3(d) + p4(d) + c1(d) + c2(d):
                cp.wait_send()
            for cp in own_out(d):
                cp.wait()
            if ar['kind'] == 'attn':
                h_out(d).wait()
        if ar['do'] != 'ag':
            for cp in p1(d) + p2(d):
                cp.wait_send()

    phase_sets = {'full': (ar_phase1, ar_phase2, ar_phase3, ar_phase4, ar_phase5, ar_phase6), 'rs': (ar_phase1, ar_phase2, ar_phase3),
                  'ag': (ar_phase3, ar_phase4, ar_phase5, ar_phase6)}

    def run_phases(k):
        for d, ar in zip(ar_in, ars):
            for when, phase in zip(ar['steps'], phase_sets[ar['do']]):
                if when == k:
                    phase(d, ar)

    def w_copies(j, n):
        slot = lax.rem(j, 2)
        cols = pl.ds(j * ffn_tile if isinstance(j, int) else pl.multiple_of(j * ffn_tile, ffn_tile), n)
        return [lcopy(w_sem.at[slot, 0], wg_hbm.at[:, cols], wbuf.at[slot, :, pl.ds(0, n)]),
                lcopy(w_sem.at[slot, 1], wu_hbm.at[:, cols], wbuf.at[slot, :, pl.ds(n, n)])]

    def lhs_copies():
        return [lcopy(lhs_sem.at[0], lhs_hbm, lhs)]

    def tile_copies(ci, j, slot):
        n = obuf.shape[2]
        cols = pl.ds(pl.multiple_of(j * n, n), n)
        return (lcopy(o_sem.at[slot], obuf.at[slot, pl.ds(0, half)], out_own[ci].at[:, cols]),
                Lazy(lambda: pltpu.make_async_remote_copy(src_ref=obuf.at[slot, pl.ds(half, half)], dst_ref=out_rcv[ci].at[:, cols],
                                             send_sem=os_sem.at[slot], recv_sem=or_sem.at[ci], device_id=core, device_id_type=MESH)))

    n_steps = cfg['n_steps']
    if kind == 'head':
        x_tile, heads, first = cfg['x_tile'], cfg['heads'], cfg['chunks'][0]
        tiles = rows // x_tile
        na = cfg['na']

    def x_copies(ci):
        return [lcopy(x_sem.at[i], at(x_hbm, pl.multiple_of((first + ci) * rows + i * x_tile, x_tile), x_tile), at(m_buf, i * x_tile, x_tile)) for i in range(tiles)]

    def qkv_copies():
        kv = pl.ds(pl.multiple_of(lax.div(t, cfg['kv_share']) * 128, 128), 128)
        cut, rest = na * 128, (heads - na) * 128
        return [lcopy(w_sem.at[0], wq_hbm.at[:, pl.ds(0, cut)], w_a), lcopy(w_sem.at[1], wq_hbm.at[:, pl.ds(cut, rest)], w_b.at[:, pl.ds(0, rest)]),
                lcopy(w_sem.at[2], wk_hbm.at[:, kv], w_b.at[:, pl.ds(rest, 128)]), lcopy(w_sem.at[3], wv_hbm.at[:, kv], w_b.at[:, pl.ds(rest + 128, 128)])]

    def norm_step(ci):
        per_tile = x_tile // 16

        def norm_rows(i, _):
            @pl.when(lax.rem(i, per_tile) == 0)
            def _():
                tile = lax.div(i, per_tile)
                dst = at(m_buf, pl.multiple_of(tile * x_tile, x_tile), x_tile)
                lcopy(x_sem.at[tile], at(x_hbm, pl.multiple_of((first + ci) * rows + tile * x_tile, x_tile), x_tile), dst).wait()
            here = pl.ds(pl.multiple_of(i * 16, 16), 16)
            val = m_buf[here, :].astype(F32)
            mean_sq = jnp.sum(val * val, axis=-1, keepdims=True) / width
            m_buf[here, :] = (val * lax.rsqrt(mean_sq + EPSILON) * norm_ref[...].astype(F32)).astype(BF16)
            return 0
        lax.fori_loop(0, rows // 16, norm_rows, 0)

    def rotate(val, gain_ref):
        val = val * lax.rsqrt(jnp.sum(val * val, axis=-1, keepdims=True) / 128 + EPSILON) * gain_ref[...].astype(F32)
        return (val * cos_ref[...] + pltpu.roll(val, 64, 1) * sin_ref[...]).astype(BF16)

    def masked(ci, val):
        row = lax.broadcasted_iota(jnp.int32, (rows, 128), 0)
        return jnp.where(row < len_ref[first + ci], val.astype(F32), 0.0).astype(BF16)

    def query_step():
        proj = jnp.dot(m_buf[...], w_a[...], preferred_element_type=F32)
        for i in range(na):
            q_buf[i] = rotate(proj[:, i * 128:(i + 1) * 128], qg_ref)

    def last_step(ci):
        proj = jnp.dot(m_buf[...], w_b[...], preferred_element_type=F32)
        for i in range(na, heads):
            q_buf[i] = rotate(proj[:, (i - na) * 128:(i - na + 1) * 128], qg_ref)
        rest = (heads - na) * 128
        key = rotate(proj[:, rest:rest + 128], kg_ref)
        k_buf[...] = key
        kc_ref[...] = masked(ci, key)
        val = proj[:, rest + 128:].astype(BF16)
        v_buf[...] = val
        vc_ref[...] = masked(ci, val)

    def attention_step(ci, h):
        length = len_ref[first + ci]
        for i in range(tiles):
            n = (i + 1) * x_tile
            q = q_buf[h, i * x_tile:n, :]
            scores = lax.dot_general(q, k_buf[:n, :], (((1,), (1,)), ((), ())), preferred_element_type=F32) * 128 ** -0.5
            row = lax.broadcasted_iota(jnp.int32, (x_tile, n), 0) + i * x_tile
            col = lax.broadcasted_iota(jnp.int32, (x_tile, n), 1)
            scores = jnp.where((col <= row) & (col < length), scores, -1e30)
            weight = jnp.exp(scores - jnp.max(scores, axis=-1, keepdims=True))
            weight = (weight * (1.0 / jnp.sum(weight, axis=-1, keepdims=True))).astype(BF16)
            out = jnp.dot(weight, v_buf[:n, :], preferred_element_type=F32).astype(BF16)
            o_buf[i * x_tile:n, pl.ds(pl.multiple_of(h * 128, 128), 128)] = out

    def order_rows():
        for s in range(16):
            src = pl.ds(pl.multiple_of(origin_block(t, s) * piece, 16), piece)
            lhs[s * piece:(s + 1) * piece, :] = o_buf[src, :]

    @pl.when(step == 0)
    def _():
        for d, ar in zip(ar_in, ars):
            for cp in ([] if ar['source'] is not None else sum_loads(d, ar)) + row_loads(d, ar):
                cp.start()
        if kind == 'mlp':
            for cp in lhs_copies() + w_copies(0, ffn_tile):
                cp.start()
        if kind == 'head':
            for cp in x_copies(0) + qkv_copies():
                cp.start()
        barrier = pltpu.get_barrier_semaphore()
        for dev in (core, xn, yn):
            pl.semaphore_signal(barrier, inc=1, device_id=dev, device_id_type=MESH)
        pl.semaphore_wait(barrier, 3)
        run_phases(0)
        if kind == 'mlp':
            for cp in lhs_copies():
                cp.wait()

    for k in sorted({k for ar in ars for k in ar['steps']} - {0, END}):
        @pl.when(step == k)
        def _(k=k):
            run_phases(k)

    def drain(ci):
        for j in (cfg['per'] - 2, cfg['per'] - 1):
            a, b = tile_copies(ci, j, j % 2)
            a.wait()
            b.wait_send()
        pltpu.make_async_copy(out_rcv[ci], out_rcv[ci], or_sem.at[ci]).wait()

    def store_tile(ci, j, value):
        slot = lax.rem(j, 2)

        @pl.when(j >= 2)
        def _():
            a, b = tile_copies(ci, j, slot)
            a.wait()
            b.wait_send()
        obuf[slot] = value
        a, b = tile_copies(ci, j, slot)
        a.start()
        b.start()

    if kind == 'mlp':
        n_up = cfg['n_up']

        n_full, rest = cfg['n_full'], cfg['rest']

        @pl.when(step + 1 < n_full)
        def _():
            for cp in w_copies(step + 1, ffn_tile):
                cp.start()

        def gate_up(j, n):
            for cp in w_copies(j, n):
                cp.wait()
            both = jnp.dot(lhs[...], wbuf[lax.rem(j, 2), :, :2 * n], preferred_element_type=F32)
            gate = both[:, :n]
            gated[:, pl.ds(j * ffn_tile if isinstance(j, int) else pl.multiple_of(j * ffn_tile, ffn_tile), n)] = (gate * jax.nn.sigmoid(gate) * both[:, n:]).astype(BF16)

        if rest:
            @pl.when(step == n_full - 1)
            def _():
                for cp in w_copies(n_full, rest):
                    cp.start()

        @pl.when(step < n_full)
        def _():
            gate_up(step, ffn_tile)
        if rest:
            @pl.when(step == n_full)
            def _():
                gate_up(n_full, rest)

        @pl.when(step >= n_up)
        def _():
            store_tile(0, step - n_up, jnp.dot(gated[...], wd_ref[...], preferred_element_type=F32).astype(BF16))
    elif kind == 'head':
        per = cfg['per']
        ci = lax.div(step, cfg['chunk_steps'])
        sub = lax.rem(step, cfg['chunk_steps'])
        for c in range(n_chunks - 1):
            @pl.when(step == (c + 1) * cfg['chunk_steps'])
            def _(c=c):
                drain(c)
                for d, ar in zip(ar_in, ars):
                    if ar['source'] == c:
                        for cp in sum_loads(d, ar):
                            cp.start()

        begin = 2

        @pl.when(sub == 0)
        def _():
            norm_step(ci)
        for b, part in enumerate((slice(0, 1), slice(1, 4))):
            @pl.when(step == b)
            def _(part=part):
                for cp in qkv_copies()[part]:
                    cp.wait()
        pl.when(sub == 0)(query_step)

        @pl.when(sub == 1)
        def _():
            last_step(ci)

        @pl.when((sub == begin) & (ci + 1 < n_chunks))
        def _():
            for cp in x_copies(ci + 1):
                cp.start()

        @pl.when((sub >= begin) & (sub < begin + heads))
        def _():
            attention_step(ci, sub - begin)
        pl.when(sub == begin + heads)(order_rows)

        @pl.when(sub >= begin + heads)
        def _():
            value = jnp.dot(lhs[...], wo_ref[...], preferred_element_type=F32).astype(BF16)
            j = sub - begin - heads
            for c in range(n_chunks):
                @pl.when(ci == c)
                def _(c=c):
                    store_tile(c, j, value)

    @pl.when(step == n_steps - 1)
    def _():
        if n_chunks:
            drain(n_chunks - 1)
        for phase in (ar_phase1, ar_phase2, ar_phase3, ar_phase4, ar_phase5, ar_phase6):
            for d, ar in zip(ar_in, ars):
                for when, own_phase in zip(ar['steps'], phase_sets[ar['do']]):
                    if when == END and own_phase is phase:
                        phase(d, ar)
        for d, ar in zip(ar_in, ars):
            ar_end(d, ar)


def run_stage(cid, kind, compute, ars, rows, width, chunks=(), kv_share=1):
    any_spec = pl.BlockSpec(memory_space=pl.ANY)
    half, quarter, piece = rows // 2, rows // 8, rows // 16
    args, in_specs, out_shape, scratch = [], [], [], []
    out_tile = 512 if width % 512 == 0 else 128
    per = width // out_tile
    cfg = dict(kind=kind, width=width, rows=rows, chunks=chunks, per=per, ffn_tile=256,
               ars=[{k: a[k] for k in ('kind', 'chunk', 'do', 'steps', 'source')} for a in ars])
    if kind == 'mlp':
        n2, wg, wu, wd = compute
        ffn = wd.shape[0]
        n_full, rest = ffn // 256, ffn % 256
        n_up = n_full + (rest > 0)
        cfg.update(n_up=n_up, n_full=n_full, rest=rest, n_steps=n_up + per)
        args += [n2, wg, wu, wd]
        in_specs += [any_spec] * 3 + [pl.BlockSpec((ffn, out_tile), lambda j: (0, jnp.maximum(j - n_up, 0)))]
        scratch += [pltpu.VMEM((rows, width), BF16), pltpu.SemaphoreType.DMA((1,)), pltpu.VMEM((rows, ffn), BF16), pltpu.VMEM((2, width, 512), BF16), pltpu.SemaphoreType.DMA((2, 2))]
    elif kind == 'head':
        lengths, tokens, wq, wk, wv, norm, q_gain, k_gain, cosine, sine, wo = compute
        x_tile = rows // 3
        heads = wq.shape[1] // 128
        out_tile = 1024 if width % 1024 == 0 else out_tile
        per = width // out_tile
        begin = 2
        na = heads - 1
        chunk_steps = begin + heads + per
        first = chunks[0]
        cfg.update(n_steps=chunk_steps * len(chunks), x_tile=x_tile, heads=heads, chunk_steps=chunk_steps, kv_share=kv_share, per=per, na=na)
        args += [lengths, tokens, wq, wk, wv, norm, q_gain, k_gain, cosine, sine, wo]
        table = pl.BlockSpec((rows, 128), lambda j: (first + lax.div(j, chunk_steps), 0))
        gain_spec = pl.BlockSpec((1, 128), lambda j: (0, 0))
        in_specs += [pl.BlockSpec(memory_space=pltpu.SMEM)] + [any_spec] * 4 + [pl.BlockSpec((1, width), lambda j: (0, 0)), gain_spec, gain_spec, table, table,
                     pl.BlockSpec((heads * 128, out_tile), lambda j: (0, jnp.maximum(lax.rem(j, chunk_steps) - begin - heads, 0)))]
        scratch += [pltpu.VMEM((rows, heads * 128), BF16), pltpu.SemaphoreType.DMA((3,)), pltpu.VMEM((rows, width), BF16),
                    pltpu.VMEM((width, na * 128), BF16), pltpu.VMEM((width, (heads - na) * 128 + 256), BF16), pltpu.SemaphoreType.DMA((4,)),
                    pltpu.VMEM((heads, rows, 128), BF16), pltpu.VMEM((rows, 128), BF16), pltpu.VMEM((rows, 128), BF16), pltpu.VMEM((rows, heads * 128), BF16)]
        cache_spec = pl.BlockSpec((rows, 128), lambda j: (lax.div(j, chunk_steps), 0))
    else:
        cfg.update(n_steps=3)
    if chunks:
        scratch += [pltpu.VMEM((2, rows, out_tile), BF16), pltpu.SemaphoreType.DMA((2,)),
                    pltpu.SemaphoreType.DMA((2,)), pltpu.SemaphoreType.DMA((len(chunks),))]
    for a in ars:
        names = (() if a['do'] == 'ag' or a['source'] is not None else ('own', 'rcv')) + (('sum',) if a['do'] == 'ag' else ()) + (() if a['do'] == 'rs' else ('res',))
        args += [a[k] for k in names]
        in_specs += [any_spec] * len(names)
        if a['kind'] == 'attn' and a['do'] != 'rs':
            args.append(a['gain'])
            in_specs.append(pl.BlockSpec((1, width), lambda j: (0, 0)))
        sizes = dict(s=(half, width), r=(half, width), r1=(2, quarter, width), r2=(2, piece, width), x=(quarter, width), n=(quarter, width))
        counts = dict(send=18, recv=18, loc=12)
        scratch += [pltpu.VMEM(sizes[k], BF16) if k in sizes else pltpu.SemaphoreType.DMA((counts[k],)) for k in ar_scratch(a['do'])]
    for _ in chunks:
        out_shape += [jax.ShapeDtypeStruct((half, width), BF16)] * 2
    out_specs = [any_spec] * len(out_shape)
    if kind == 'head':
        out_shape += [jax.ShapeDtypeStruct((rows * len(chunks), 128), BF16)] * 2
        out_specs += [cache_spec] * 2
    for a in ars:
        if a['do'] == 'rs':
            out_shape.append(jax.ShapeDtypeStruct((quarter, width), BF16))
            continue
        out_shape.append(jax.ShapeDtypeStruct((rows, width), BF16))
        if a['kind'] == 'attn':
            out_shape.append(jax.ShapeDtypeStruct((quarter, width), BF16))
    return pl.pallas_call(
        functools.partial(stage_kernel, cfg),
        grid=(cfg['n_steps'],),
        out_shape=out_shape,
        in_specs=in_specs,
        out_specs=out_specs + [any_spec] * (len(out_shape) - len(out_specs)),
        scratch_shapes=scratch,
        compiler_params=pltpu.CompilerParams(collective_id=cid, has_side_effects=True, vmem_limit_bytes=62 * 1024 * 1024,
                                             dimension_semantics=('arbitrary',)),
        name=f'stage{cid}',
    )(*args)


def place_kernel(n, table_ref, *refs):
    for b in range(n):
        refs[n][b] = refs[b][...]


def place_rows(chunks, rows, width):
    t = lax.axis_index('tp')
    piece = rows // 16
    blocks = jnp.stack([jnp.asarray(origin_block(t, s), jnp.int32) for s in range(16)])
    table = jnp.argmax(blocks[None, :] == jnp.arange(16, dtype=jnp.int32)[:, None], axis=1).astype(jnp.int32)
    n = len(chunks)
    return pl.pallas_call(
        functools.partial(place_kernel, n),
        grid_spec=pltpu.PrefetchScalarGridSpec(
            num_scalar_prefetch=1, grid=(16,),
            in_specs=[pl.BlockSpec((piece, width), lambda k, tab: (tab[k], 0))] * n,
            out_specs=pl.BlockSpec((n, piece, width), lambda k, tab: (0, k, 0))),
        out_shape=jax.ShapeDtypeStruct((n, rows, width), BF16),
        name='place',
    )(table, *chunks)


def layer_body(tokens, positions, lengths, norm_attn, norm_mlp, q_gain, k_gain, w_query, w_key, w_value, w_out, w_gate, w_up, w_down, tp_size):
    num_prompts, seq_len, hidden_dim = tokens.shape
    head_dim = q_gain.shape[0]
    kv_heads = w_key.shape[1] // head_dim
    rows_n = num_prompts * seq_len
    tokens_flat = tokens.reshape(rows_n, hidden_dim)
    cosine, sine = rope_tables(positions, head_dim // 2)
    head_in = (lengths, tokens_flat, w_query, w_key, w_value, norm_attn.reshape(1, hidden_dim), q_gain.reshape(1, head_dim), k_gain.reshape(1, head_dim), cosine, sine, w_out)

    gain = norm_mlp.reshape(1, hidden_dim)
    stage = functools.partial(run_stage, rows=seq_len, width=hidden_dim, kv_share=tp_size // kv_heads)

    def attn_ar(do, chunk, steps, source=None, **arrays):
        return dict(kind='attn', do=do, chunk=chunk, steps=steps, source=source, res=tokens_flat, gain=gain, **arrays)

    def mlp_ar(steps, own, rcv, hid):
        return dict(kind='mlp', do='full', chunk=0, steps=steps, source=None, own=own, rcv=rcv, res=hid)

    weights = (w_gate, w_up, w_down)
    own0, rcv0, kc0, vc0 = stage(1, 'head', head_in, [], chunks=(0,))
    _, _, own2, rcv2, kc1, vc1, n0, h0, sum1 = stage(2, 'head', head_in, [
        attn_ar('full', 0, (0, 1, 9, 13, 15, 18), own=own0, rcv=rcv0), attn_ar('rs', 1, (13, 19, END), source=0)], chunks=(1, 2))
    m_own0, m_rcv0, sum2, n1, h1 = stage(3, 'mlp', (n0, *weights), [
        attn_ar('rs', 2, (0, 2, END), own=own2, rcv=rcv2), attn_ar('ag', 1, (0, 6, END, END), sum=sum1)], chunks=(0,))
    m_own1, m_rcv1, out0, n2, h2 = stage(4, 'mlp', (n1, *weights), [
        mlp_ar((0, 2, 10, END, END, END), m_own0, m_rcv0, h0), attn_ar('ag', 2, (0, 6, END, END), sum=sum2)], chunks=(1,))
    m_own2, m_rcv2, out1 = stage(5, 'mlp', (n2, *weights), [mlp_ar((0, 2, 7, 11, END, END), m_own1, m_rcv1, h1)], chunks=(2,))
    out2, = stage(6, 'none', (), [mlp_ar((0, 0, 1, 2, END, END), m_own2, m_rcv2, h2)])
    k_parts, v_parts = [kc0, kc1], [vc0, vc1]
    cache_shape = (num_prompts, seq_len, 1, head_dim)
    k_cache = jnp.concatenate(k_parts).reshape(cache_shape)
    v_cache = jnp.concatenate(v_parts).reshape(cache_shape)
    output = place_rows([out0, out1, out2], seq_len, hidden_dim)
    return output, k_cache, v_cache


def solution(mesh):
    body = functools.partial(layer_body, tp_size=mesh.shape['tp'])
    in_specs = (P('dp', None, None), P('dp', None), P('dp'), P(), P(), P(), P(), P(None, 'tp'), P(), P(), P('tp', None), P(None, 'tp'), P(None, 'tp'), P('tp', None))
    out_specs = (P('dp', None, None), P('dp', None, 'tp', None), P('dp', None, 'tp', None))
    return jax.shard_map(body, mesh=mesh, in_specs=in_specs, out_specs=out_specs, check_vma=False)
```
